32 devices in a mesh: groups: 2 (over x), feat: 16 (over z, y, core).
Axes of the slice: x: 2, y: 2, z: 4, core: 2. Of those that a mesh axis runs over, the one named last changes fastest.
Arguments:
- cells: bfloat16 [96, 512, 192], P('groups', 'feat'), parts along dimension 0, may hold values from -6 to 6
- missing: int32 [96, 512], P('groups', 'feat'), parts along dimension 0, may hold values 0 or 1
- feat_ids: int32 [1024], P(('groups', 'feat')), parts along dimension 0, may hold values from 0 to 63
- feat_table: float32 [64, 192], replicated, may hold values from -5 to 5
- nan_embed: float32 [192], replicated, may hold values from -5 to 5
- gain_one: float32 [192], replicated, may hold values from 0.1 to 1.9
- w_qkv: bfloat16 [192, 576], replicated, may hold values from -3 to 3
- w_out: bfloat16 [192, 192], replicated, may hold values from -0.4375 to 0.4375
- gain_two: float32 [192], replicated, may hold values from 0.1 to 1.9
- w_up: bfloat16 [192, 768], replicated, may hold values from -0.4375 to 0.4375
- w_down: bfloat16 [768, 192], replicated, may hold values from -0.21875 to 0.21875
Outputs:
- result: float32 [96, 512, 192], P('groups', 'feat'), parts along dimension 0
The draws below stay inside these ranges and needn't reach their ends.
There are 2 independent parts, one for each index of `groups`. The reference program is written for one: setup_inputs(seed, part) draws one part's arguments, and reference() takes and returns one part's arrays. A program takes and returns all parts, laid end to end along the dimension named above; an argument that names none is the same for every part. Nothing has to cross between parts.
All inputs are finite; a program needn't handle non-finite values. No bound on the sum of `missing` on one device may be relied on, other than what follows from the above.
Results may differ from the reference program's by a relative error of at most 0.007.
The reference program's roundings to bfloat16 on the way (of `tokens`, `normed`, `qkv`, `probs`, `context`, `normed_two` and `act`) count: a program that leaves them out, or rounds other values in their place, can miss the bound.
Values may be sent and summed in bfloat16 or wider, within the bound.
A program may use at most 64 MiB of HBM per device.

```python
import jax
import jax.numpy as jnp
from jax import lax

E = 192
HEADS = 6
MLP = 768
F = 512
NCAT = 64
R = 48


def draw_w_qkv(key, part):
    weights = jax.random.normal(key, (E, 3 * E), jnp.float32) * E ** (-0.5)
    return jnp.clip(weights, -3.0, 3.0).astype(jnp.bfloat16)


def touch_ends(values, key, smallest, top_value):
    longest = values.shape.index(max(values.shape))
    spots = []
    for shift in (0, 1):
        where = [jax.random.randint(jax.random.fold_in(key, axis), (), 0, length) for axis, length in enumerate(values.shape)]
        where[longest] = (where[longest] + shift) % values.shape[longest]
        spots.append(tuple(where))
    return values.at[spots[0]].set(smallest).at[spots[1]].set(top_value)


def block_scale(rng, extent, shards, smallest, high):
    def one(dim, parts):
        steps = jax.random.uniform(jax.random.fold_in(jax.random.fold_in(rng, 6), dim), (parts,), jnp.float32, smallest / len(shards), high / len(shards))
        return jnp.repeat(jnp.exp(steps), extent[dim] // parts).reshape((-1,) + (1,) * (len(extent) - dim - 1))

    loudness = one(*shards[0])
    for cut in shards[1:]:
        loudness = loudness * one(*cut)
    return loudness


def centred(stream_key, extent, spread, reach, pieces=(), held_as=jnp.bfloat16):
    drawn = jax.random.normal(stream_key, extent, jnp.float32) * spread
    if len(pieces) > 0:
        drawn = block_scale(stream_key, extent, pieces, -0.22, 0.18) * drawn
    return jnp.clip(drawn, min=-reach, max=reach).astype(held_as)


def setup_inputs(seed: int = 0, part: int = 0) -> dict:
    streams_of = jax.random.split(jax.random.key(seed), 12)
    part_splits = jax.random.split(jax.random.fold_in(streams_of[11], part), 12)
    return {
        "cells": centred(part_splits[0], (R, F, E), 1.0, 6.0, ((1, 16),)),
        "missing": touch_ends((jax.random.randint(part_splits[1], (R, F), 0, 4) < 1).astype(jnp.int32), jax.random.fold_in(part_splits[1], 1), 0, 1),
        "feat_ids": touch_ends(jax.random.randint(part_splits[2], (F,), 0, NCAT), jax.random.fold_in(part_splits[2], 1), 0, NCAT - 1).astype(jnp.int32),
        "feat_table": centred(streams_of[3], (NCAT, E), 0.7, 5.0, (), jnp.float32),
        "nan_embed": centred(streams_of[4], (E,), 1.0, 5.0, (), jnp.float32),
        "gain_one": jnp.clip(1.0 + 0.18 * jax.random.normal(streams_of[5], (E,), jnp.float32), 0.1, 1.9),
        "w_qkv": draw_w_qkv(jax.random.fold_in(streams_of[11], 71), part),
        "w_out": centred(streams_of[7], (E, E), E ** -0.5, 0.4375),
        "gain_two": jnp.clip(1.0 + 0.18 * jax.random.normal(streams_of[8], (E,), jnp.float32), 0.1, 1.9),
        "w_up": centred(streams_of[9], (E, MLP), E ** -0.5, 0.4375),
        "w_down": centred(streams_of[10], (MLP, E), MLP ** -0.5, 0.21875),
    }


def cell_norm(values, gain):
    mean = lax.optimization_barrier(jnp.mean(values, axis=-1, keepdims=True))
    centered = values - mean
    var = lax.optimization_barrier(jnp.mean(centered * centered, axis=-1, keepdims=True))
    return centered * lax.rsqrt(var + 1e-05) * gain

def attend(qkv):
    width = qkv.shape[-1] // 3
    count = qkv.shape[0]
    head_dim = width // HEADS
    query = qkv[:, :width].reshape(count, HEADS, head_dim).astype(jnp.float32)
    keys = qkv[:, width:2 * width].reshape(count, HEADS, head_dim).astype(jnp.float32)
    values = qkv[:, 2 * width:].reshape(count, HEADS, head_dim).astype(jnp.float32)
    scores = jnp.einsum('qhd,phd->hqp', query, keys) * head_dim ** (-0.5)
    top = lax.optimization_barrier(jnp.max(scores, axis=-1, keepdims=True))
    expo = jnp.exp(scores - top)
    probs = (expo / lax.optimization_barrier(jnp.sum(expo, axis=-1, keepdims=True))).astype(jnp.bfloat16)
    context = jnp.einsum('hqp,phd->qhd', probs.astype(jnp.float32), values)
    return context.astype(jnp.bfloat16).reshape(count, width)

def reference(cells, missing, feat_ids, feat_table, nan_embed, gain_one, w_qkv, w_out, gain_two, w_up, w_down):
    onehot = (feat_ids[:, None] == jnp.arange(NCAT, dtype=jnp.int32)[None, :]).astype(jnp.float32)
    femb = jnp.dot(onehot, feat_table, precision=lax.Precision.HIGHEST)
    tokens = (cells.astype(jnp.float32) + missing[..., None].astype(jnp.float32) * nan_embed + femb[None]).astype(jnp.bfloat16)

    def one_row(row):
        base = row.astype(jnp.float32)
        normed = cell_norm(base, gain_one).astype(jnp.bfloat16)
        qkv = jnp.dot(normed, w_qkv, preferred_element_type=jnp.float32).astype(jnp.bfloat16)
        context = attend(qkv)
        mid = base + jnp.dot(context, w_out, preferred_element_type=jnp.float32)
        normed_two = cell_norm(mid, gain_two).astype(jnp.bfloat16)
        act = jax.nn.gelu(jnp.dot(normed_two, w_up, preferred_element_type=jnp.float32), approximate=False).astype(jnp.bfloat16)
        return mid + jnp.dot(act, w_down, preferred_element_type=jnp.float32)
    return lax.map(one_row, tokens)
```

```python
import functools
import math

import jax
import jax.numpy as jnp
from jax import lax
from jax.experimental import pallas as pl
from jax.experimental.pallas import tpu as pltpu
from jax.sharding import PartitionSpec as P

HEADS = 6
MESH = pl.DeviceIdType.MESH
F32 = jnp.float32
BF16 = jnp.bfloat16


def cell_norm(values, gain):
    mean = jnp.mean(values, axis=-1, keepdims=True)
    centered = values - mean
    var = jnp.mean(centered * centered, axis=-1, keepdims=True)
    return (centered * lax.rsqrt(var + 1e-05) * gain).astype(BF16)


def pack(values, packed):
    if not packed:
        return values
    half = values.shape[-2] // 2
    tail = values[..., 128:]
    tail = jnp.concatenate([tail[..., :half, :], tail[..., half:, :]], axis=-1)
    return jnp.concatenate([values[..., :128], tail], axis=-2)


def unpack(values, feats, width, packed):
    if packed:
        rest = width - 128
        tail = values[:, feats:]
        tail = jnp.concatenate([tail[..., :rest], tail[..., rest:]], axis=-2)
        values = jnp.concatenate([values[:, :feats], tail], axis=-1)
    return values.reshape(values.shape[0] * feats, width)


def attend(normed, wk, wqv_t):
    width = wk.shape[0]
    head_dim = width // HEADS
    count = normed.shape[0]
    keys = jnp.dot(normed, wk, preferred_element_type=F32).astype(BF16)
    turned = lax.dot_general(
        wqv_t, normed, (((1,), (1,)), ((), ())), preferred_element_type=F32
    ).astype(BF16)
    scale = head_dim ** (-0.5) * math.log2(math.e)
    ones = jnp.ones((16, count), BF16)
    outs = []
    for head in range(HEADS):
        low = head * head_dim
        block = low // 128 * 128
        high = min(block + 128, width)
        parts = []
        if low > block:
            parts.append(jnp.zeros((low - block, count), BF16))
        parts.append(turned[low : low + head_dim])
        if high > low + head_dim:
            parts.append(jnp.zeros((high - low - head_dim, count), BF16))
        query = jnp.concatenate(parts, axis=0)
        scores = jnp.dot(keys[:, block:high], query, preferred_element_type=F32)
        top = jnp.max(scores, axis=0, keepdims=True)
        expo = jnp.exp2((scores - top) * scale).astype(BF16)
        values = jnp.concatenate([turned[width + low : width + low + head_dim], ones], axis=0)
        sums = jnp.dot(values, expo, preferred_element_type=F32)
        outs.append(sums[:head_dim] / sums[head_dim : head_dim + 1])
    return jnp.concatenate(outs, axis=0).T


def kernel(
    n, rows, feats, width, packed,
    cells, missing, feat_ids, feat_table, nan_embed, gain_one, w_qkv, w_out, gain_two, w_up, w_down,
    out, tok, got, ctx, back, wqv_t, send_sems, recv_sems,
):
    me = lax.axis_index("feat")
    barrier = pltpu.get_barrier_semaphore()

    def greet(step, carry):
        peer = lax.rem(me + step, n)
        pl.semaphore_signal(barrier, inc=1, device_id={"feat": peer}, device_id_type=MESH)
        return carry

    lax.fori_loop(1, n, greet, 0)

    ncat = feat_table.shape[0]
    hot = (lax.broadcasted_iota(jnp.int32, (ncat, feats), 0) == feat_ids[...]).astype(F32)
    femb = lax.dot_general(
        hot, feat_table[...], (((0,), (0,)), ((), ())),
        precision=lax.Precision.HIGHEST, preferred_element_type=F32,
    )
    nan = nan_embed[...]
    absent = missing[...].astype(F32)[:, :, None].reshape(n, rows, feats, 1)
    for row in range(rows):
        values = cells[:, row].astype(F32)
        values = (values + absent[:, row] * nan[None] + femb[None]).astype(BF16)
        tok[row] = pack(values, packed)

    pl.semaphore_wait(barrier, n - 1)

    def spread(source, target, kind, row):
        def one(step, carry):
            peer = lax.rem(me + step, n)
            pltpu.make_async_remote_copy(
                src_ref=source.at[row, peer],
                dst_ref=target.at[row, me],
                send_sem=send_sems.at[kind, row],
                recv_sem=recv_sems.at[kind, row],
                device_id={"feat": peer},
                device_id_type=MESH,
            ).start()
            return carry

        lax.fori_loop(1, n, one, 0)

    def settle(ref, sems, kind, row):
        piece = ref.at[row, pl.ds(0, n - 1)]
        pltpu.make_async_copy(piece, piece, sems.at[kind, row]).wait()

    for row in range(rows):
        spread(tok, got, 0, row)
    for row in range(rows):
        got[row, pl.ds(me, 1)] = tok[row, pl.ds(me, 1)]
    wqv_t[0:width] = w_qkv[:, :width].astype(F32).T.astype(BF16)
    wqv_t[width:] = w_qkv[:, 2 * width :].astype(F32).T.astype(BF16)

    def attention(row, carry):
        settle(got, recv_sems, 0, row)
        base = unpack(got[row].astype(F32), feats, width, packed)
        normed = cell_norm(base, gain_one[...])
        context = attend(normed, w_qkv[:, width : 2 * width], wqv_t[...])
        sent = pack(context.reshape(n, feats, width), packed).astype(BF16)
        ctx[row] = sent
        spread(ctx, back, 1, row)
        back[row, pl.ds(me, 1)] = ctx[row, pl.ds(me, 1)]
        return carry

    lax.fori_loop(0, rows, attention, 0)

    def finish(row, carry):
        settle(back, recv_sems, 1, row)
        context = unpack(back[row].astype(F32), feats, width, packed).astype(BF16)
        base = unpack(tok[row].astype(F32), feats, width, packed)
        mid = base + jnp.dot(context, w_out[...], preferred_element_type=F32)
        normed = cell_norm(mid, gain_two[...])
        hidden = jnp.dot(normed, w_up[...], preferred_element_type=F32)
        act = (0.5 * hidden * (1.0 + lax.erf(hidden * math.sqrt(0.5)))).astype(BF16)
        result = mid + jnp.dot(act, w_down[...], preferred_element_type=F32)
        out[:, pl.ds(row, 1)] = result.reshape(n, 1, feats, width)
        return carry

    lax.fori_loop(0, rows, finish, 0)

    for row in range(rows):
        settle(tok, send_sems, 0, row)
        settle(ctx, send_sems, 1, row)


def body(
    cells, missing, feat_ids, feat_table, nan_embed, gain_one, w_qkv, w_out, gain_two, w_up, w_down
):
    n = lax.axis_size("feat")
    all_rows, feats, width = cells.shape
    rows = all_rows // n
    packed = width == 192 and feats % 32 == 0
    piece = (feats + feats // 2, 128) if packed else (feats, width)
    buffer = pltpu.VMEM((rows, n) + piece, BF16)
    result = pl.pallas_call(
        functools.partial(kernel, n, rows, feats, width, packed),
        out_shape=jax.ShapeDtypeStruct((n, rows, feats, width), F32),
        in_specs=[pl.BlockSpec(memory_space=pltpu.VMEM)] * 11,
        out_specs=pl.BlockSpec(memory_space=pltpu.VMEM),
        scratch_shapes=[
            buffer,
            buffer,
            buffer,
            buffer,
            pltpu.VMEM((2 * width, width), BF16),
            pltpu.SemaphoreType.DMA((2, rows)),
            pltpu.SemaphoreType.DMA((2, rows)),
        ],
        compiler_params=pltpu.CompilerParams(
            collective_id=0, has_side_effects=True, vmem_limit_bytes=60 * 1024 * 1024
        ),
    )(
        cells.reshape(n, rows, feats, width),
        missing,
        feat_ids[None],
        feat_table,
        nan_embed[None],
        gain_one[None],
        w_qkv,
        w_out,
        gain_two[None],
        w_up,
        w_down,
    )
    return result.reshape(all_rows, feats, width)


def solution(mesh):
    in_specs = (
        P("groups", "feat", None),
        P("groups", "feat"),
        P(("groups", "feat")),
        P(),
        P(),
        P(),
        P(),
        P(),
        P(),
        P(),
        P(),
    )
    out_specs = P("groups", "feat", None)
    return jax.shard_map(body, mesh=mesh, in_specs=in_specs, out_specs=out_specs, check_vma=False)
```

```python
import functools
import math

import jax
import jax.numpy as jnp
from jax import lax
from jax.experimental import pallas as pl
from jax.experimental.pallas import tpu as pltpu
from jax.sharding import PartitionSpec as P

HEADS = 6
MESH = pl.DeviceIdType.MESH
F32 = jnp.float32
BF16 = jnp.bfloat16
LIMIT = 60 * 1024 * 1024


def cell_norm(values, gain):
    mean = jnp.mean(values, axis=-1, keepdims=True)
    centered = values - mean
    var = jnp.mean(centered * centered, axis=-1, keepdims=True)
    return (centered * lax.rsqrt(var + 1e-05) * gain).astype(BF16)


def pack(values, packed):
    if not packed:
        return values
    half = values.shape[-2] // 2
    tail = values[..., 128:]
    tail = jnp.concatenate([tail[..., :half, :], tail[..., half:, :]], axis=-1)
    return jnp.concatenate([values[..., :128], tail], axis=-2)


def unpack(values, feats, width, packed):
    if packed:
        rest = width - 128
        tail = values[:, feats:]
        tail = jnp.concatenate([tail[..., :rest], tail[..., rest:]], axis=-2)
        values = jnp.concatenate([values[:, :feats], tail], axis=-1)
    return values.reshape(values.shape[0] * feats, width)


def attend(normed, wk, wqv_t):
    width = wk.shape[0]
    head_dim = width // HEADS
    count = normed.shape[0]
    keys = jnp.dot(normed, wk, preferred_element_type=F32).astype(BF16)
    turned = lax.dot_general(
        wqv_t, normed, (((1,), (1,)), ((), ())), preferred_element_type=F32
    ).astype(BF16)
    scale = head_dim ** (-0.5) * math.log2(math.e)
    ones = jnp.ones((16, count), BF16)
    outs = []
    for head in range(HEADS):
        low = head * head_dim
        block = low // 128 * 128
        high = min(block + 128, width)
        parts = []
        if low > block:
            parts.append(jnp.zeros((low - block, count), BF16))
        parts.append(turned[low : low + head_dim])
        if high > low + head_dim:
            parts.append(jnp.zeros((high - low - head_dim, count), BF16))
        query = jnp.concatenate(parts, axis=0)
        scores = jnp.dot(keys[:, block:high], query, preferred_element_type=F32)
        top = jnp.max(scores, axis=0, keepdims=True)
        expo = jnp.exp2((scores - top) * scale).astype(BF16)
        values = jnp.concatenate([turned[width + low : width + low + head_dim], ones], axis=0)
        sums = jnp.dot(values, expo, preferred_element_type=F32)
        outs.append(sums[:head_dim] / sums[head_dim : head_dim + 1])
    return jnp.concatenate(outs, axis=0).T


def kernel(n, rows, feats, width, packed, *refs):
    sources, refs = refs[:11], refs[11:]
    out, held, refs = refs[0], refs[1:12], refs[12:]
    tok, got, ctx, back, wqv_t, done, load_sems, send_sems, recv_sems, out_sems = refs
    (cells, missing, feat_ids, feat_table, nan_embed) = held[:5]
    (gain_one, w_qkv, w_out, gain_two, w_up, w_down) = held[5:]
    me = lax.axis_index("feat")
    barrier = pltpu.get_barrier_semaphore()

    def greet(step, carry):
        peer = lax.rem(me + step, n)
        pl.semaphore_signal(barrier, inc=1, device_id={"feat": peer}, device_id_type=MESH)
        return carry

    lax.fori_loop(1, n, greet, 0)

    loads = [
        pltpu.make_async_copy(source, target, load_sems.at[spot])
        for spot, (source, target) in enumerate(zip(sources, held))
    ]
    for load in loads:
        load.start()
    for load in loads[:5]:
        load.wait()

    ncat = feat_table.shape[0]
    hot = (lax.broadcasted_iota(jnp.int32, (ncat, feats), 0) == feat_ids[...]).astype(F32)
    femb = lax.dot_general(
        hot, feat_table[...], (((0,), (0,)), ((), ())),
        precision=lax.Precision.HIGHEST, preferred_element_type=F32,
    )
    nan = nan_embed[...]
    absent = missing[...].astype(F32)
    for row in range(rows):
        for peer in range(n):
            spot = peer * rows + row
            values = cells[peer, row].astype(F32)
            values = (values + absent[:, spot : spot + 1] * nan + femb).astype(BF16)
            tok[row, peer] = pack(values, packed)
    for row in range(rows):
        got[row, pl.ds(me, 1)] = tok[row, pl.ds(me, 1)]
    for load in loads[5:]:
        load.wait()
    wqv_t[0:width] = w_qkv[:, :width].astype(F32).T.astype(BF16)
    wqv_t[width:] = w_qkv[:, 2 * width :].astype(F32).T.astype(BF16)

    pl.semaphore_wait(barrier, n - 1)

    def spread(source, target, kind, row):
        def one(step, carry):
            peer = lax.rem(me + step, n)
            pltpu.make_async_remote_copy(
                src_ref=source.at[row, peer],
                dst_ref=target.at[row, me],
                send_sem=send_sems.at[kind, row],
                recv_sem=recv_sems.at[kind, row],
                device_id={"feat": peer},
                device_id_type=MESH,
            ).start()
            return carry

        lax.fori_loop(1, n, one, 0)

    def settle(ref, sems, kind, row):
        piece = ref.at[row, pl.ds(0, n - 1)]
        pltpu.make_async_copy(piece, piece, sems.at[kind, row]).wait()

    for row in range(rows):
        spread(tok, got, 0, row)

    def attention(row, carry):
        settle(got, recv_sems, 0, row)
        base = unpack(got[row].astype(F32), feats, width, packed)
        normed = cell_norm(base, gain_one[...])
        context = attend(normed, w_qkv[:, width : 2 * width], wqv_t[...])
        sent = pack(context.reshape(n, feats, width), packed).astype(BF16)
        ctx[row] = sent
        spread(ctx, back, 1, row)
        back[row, pl.ds(me, 1)] = ctx[row, pl.ds(me, 1)]
        return carry

    lax.fori_loop(0, rows, attention, 0)

    def store(row):
        return pltpu.make_async_copy(done.at[row], out.at[:, row], out_sems.at[row])

    def finish(row, carry):
        settle(back, recv_sems, 1, row)
        context = unpack(back[row].astype(F32), feats, width, packed).astype(BF16)
        base = unpack(tok[row].astype(F32), feats, width, packed)
        mid = base + jnp.dot(context, w_out[...], preferred_element_type=F32)
        normed = cell_norm(mid, gain_two[...])
        hidden = jnp.dot(normed, w_up[...], preferred_element_type=F32)
        act = (0.5 * hidden * (1.0 + lax.erf(hidden * math.sqrt(0.5)))).astype(BF16)
        result = mid + lax.dot_general(
            act, w_down[...], (((1,), (1,)), ((), ())), preferred_element_type=F32
        )
        done[row] = result.reshape(n, feats, width)
        store(row).start()
        return carry

    lax.fori_loop(0, rows, finish, 0)

    for row in range(rows):
        settle(tok, send_sems, 0, row)
        settle(ctx, send_sems, 1, row)
        store(row).wait()


def body(
    cells, missing, feat_ids, feat_table, nan_embed, gain_one, w_qkv, w_out, gain_two, w_up, w_down
):
    n = lax.axis_size("feat")
    all_rows, feats, width = cells.shape
    rows = all_rows // n
    packed = width == 192 and feats % 32 == 0
    piece = (feats + feats // 2, 128) if packed else (feats, width)
    buffer = pltpu.VMEM((rows, n) + piece, BF16)
    operands = (
        cells.reshape(n, rows, feats, width),
        missing.T,
        feat_ids[None],
        feat_table,
        nan_embed[None],
        gain_one[None],
        w_qkv,
        w_out,
        gain_two[None],
        w_up,
        w_down.T,
    )
    result = pl.pallas_call(
        functools.partial(kernel, n, rows, feats, width, packed),
        out_shape=jax.ShapeDtypeStruct((n, rows, feats, width), F32),
        in_specs=[pl.BlockSpec(memory_space=pltpu.HBM)] * len(operands),
        out_specs=pl.BlockSpec(memory_space=pltpu.HBM),
        scratch_shapes=[pltpu.VMEM(x.shape, x.dtype) for x in operands]
        + [
            buffer,
            buffer,
            buffer,
            buffer,
            pltpu.VMEM((2 * width, width), BF16),
            pltpu.VMEM((rows, n, feats, width), F32),
            pltpu.SemaphoreType.DMA((len(operands),)),
            pltpu.SemaphoreType.DMA((2, rows)),
            pltpu.SemaphoreType.DMA((2, rows)),
            pltpu.SemaphoreType.DMA((rows,)),
        ],
        compiler_params=pltpu.CompilerParams(
            collective_id=0, has_side_effects=True, vmem_limit_bytes=LIMIT
        ),
    )(*operands)
    return result.reshape(all_rows, feats, width)


def solution(mesh):
    in_specs = (
        P("groups", "feat", None),
        P("groups", "feat"),
        P(("groups", "feat")),
        P(),
        P(),
        P(),
        P(),
        P(),
        P(),
        P(),
        P(),
    )
    out_specs = P("groups", "feat", None)
    return jax.shard_map(body, mesh=mesh, in_specs=in_specs, out_specs=out_specs, check_vma=False)
```

```python
import functools
import math

import jax
import jax.numpy as jnp
from jax import lax
from jax.experimental import pallas as pl
from jax.experimental.pallas import tpu as pltpu
from jax.sharding import PartitionSpec as P

HEADS = 6
MESH = pl.DeviceIdType.MESH
F32 = jnp.float32
BF16 = jnp.bfloat16
LIMIT = 60 * 1024 * 1024


def cell_norm(values, gain):
    mean = jnp.mean(values, axis=-1, keepdims=True)
    centered = values - mean
    var = jnp.mean(centered * centered, axis=-1, keepdims=True)
    return (centered * lax.rsqrt(var + 1e-05) * gain).astype(BF16)


def pack(values, packed):
    if not packed:
        return values
    half = values.shape[-2] // 2
    tail = values[..., 128:]
    tail = jnp.concatenate([tail[..., :half, :], tail[..., half:, :]], axis=-1)
    return jnp.concatenate([values[..., :128], tail], axis=-2)


def unpack(values, feats, width, packed):
    if packed:
        rest = width - 128
        tail = values[:, feats:]
        tail = jnp.concatenate([tail[..., :rest], tail[..., rest:]], axis=-2)
        values = jnp.concatenate([values[:, :feats], tail], axis=-1)
    return values.reshape(values.shape[0] * feats, width)


def attend(normed, wk, wqv_t):
    width = wk.shape[0]
    head_dim = width // HEADS
    count = normed.shape[0]
    keys = jnp.dot(normed, wk, preferred_element_type=F32).astype(BF16)
    turned = lax.dot_general(
        wqv_t, normed, (((1,), (1,)), ((), ())), preferred_element_type=F32
    ).astype(BF16)
    scale = head_dim ** (-0.5) * math.log2(math.e)
    ones = jnp.ones((16, count), BF16)
    outs = []
    for head in range(HEADS):
        low = head * head_dim
        block = low // 128 * 128
        high = min(block + 128, width)
        parts = []
        if low > block:
            parts.append(jnp.zeros((low - block, count), BF16))
        parts.append(turned[low : low + head_dim])
        if high > low + head_dim:
            parts.append(jnp.zeros((high - low - head_dim, count), BF16))
        query = jnp.concatenate(parts, axis=0)
        scores = jnp.dot(keys[:, block:high], query, preferred_element_type=F32)
        top = jnp.max(scores, axis=0, keepdims=True)
        expo = jnp.exp2((scores - top) * scale).astype(BF16)
        values = jnp.concatenate([turned[width + low : width + low + head_dim], ones], axis=0)
        sums = jnp.dot(values, expo, preferred_element_type=F32)
        outs.append(sums[:head_dim] / sums[head_dim : head_dim + 1])
    return jnp.concatenate(outs, axis=0).T


def kernel(n, rows, feats, width, packed, *refs):
    sources, refs = refs[:11], refs[11:]
    out, held, refs = refs[0], refs[1:12], refs[12:]
    tok, got, ctx, back, wqv_t, done, load_sems, send_sems, recv_sems, out_sems = refs
    (cells, missing, feat_ids, feat_table, nan_embed) = held[:5]
    (gain_one, w_qkv, w_out, gain_two, w_up, w_down) = held[5:]
    me = lax.axis_index("feat")
    barrier = pltpu.get_barrier_semaphore()

    def greet(step, carry):
        peer = lax.rem(me + step, n)
        pl.semaphore_signal(barrier, inc=1, device_id={"feat": peer}, device_id_type=MESH)
        return carry

    lax.fori_loop(1, n, greet, 0)

    loads = [
        pltpu.make_async_copy(source, target, load_sems.at[spot])
        for spot, (source, target) in enumerate(zip(sources, held))
    ]
    for load in loads:
        load.start()
    for load in loads[:5]:
        load.wait()

    ncat = feat_table.shape[0]
    hot = (lax.broadcasted_iota(jnp.int32, (ncat, feats), 0) == feat_ids[...]).astype(F32)
    femb = lax.dot_general(
        hot, feat_table[...], (((0,), (0,)), ((), ())),
        precision=lax.Precision.HIGHEST, preferred_element_type=F32,
    )
    nan = nan_embed[...]
    absent = missing[...].astype(F32)
    def spread(source, target, kind, row):
        def one(step, carry):
            peer = lax.rem(me + step, n)
            pltpu.make_async_remote_copy(
                src_ref=source.at[row, peer],
                dst_ref=target.at[row, me],
                send_sem=send_sems.at[kind, row],
                recv_sem=recv_sems.at[kind, row],
                device_id={"feat": peer},
                device_id_type=MESH,
            ).start()
            return carry

        lax.fori_loop(1, n, one, 0)

    def settle(ref, sems, kind, row):
        piece = ref.at[row, pl.ds(0, n - 1)]
        pltpu.make_async_copy(piece, piece, sems.at[kind, row]).wait()

    for row in range(rows):
        for peer in range(n):
            spot = peer * rows + row
            values = cells[peer, row].astype(F32)
            values = (values + absent[:, spot : spot + 1] * nan + femb).astype(BF16)
            tok[row, peer] = pack(values, packed)
        if row == 0:
            pl.semaphore_wait(barrier, n - 1)
        spread(tok, got, 0, row)
    for row in range(rows):
        got[row, pl.ds(me, 1)] = tok[row, pl.ds(me, 1)]
    for load in loads[5:]:
        load.wait()
    wqv_t[0:width] = w_qkv[:, :width].astype(F32).T.astype(BF16)
    wqv_t[width:] = w_qkv[:, 2 * width :].astype(F32).T.astype(BF16)

    def attention(row, carry):
        settle(got, recv_sems, 0, row)
        base = unpack(got[row].astype(F32), feats, width, packed)
        normed = cell_norm(base, gain_one[...])
        context = attend(normed, w_qkv[:, width : 2 * width], wqv_t[...])
        sent = pack(context.reshape(n, feats, width), packed).astype(BF16)
        ctx[row] = sent
        spread(ctx, back, 1, row)
        back[row, pl.ds(me, 1)] = ctx[row, pl.ds(me, 1)]
        return carry

    lax.fori_loop(0, rows, attention, 0)

    def store(row):
        return pltpu.make_async_copy(done.at[row], out.at[:, row], out_sems.at[row])

    def finish(row, carry):
        settle(back, recv_sems, 1, row)
        context = unpack(back[row].astype(F32), feats, width, packed).astype(BF16)
        base = unpack(tok[row].astype(F32), feats, width, packed)
        mid = base + jnp.dot(context, w_out[...], preferred_element_type=F32)
        normed = cell_norm(mid, gain_two[...])
        hidden = jnp.dot(normed, w_up[...], preferred_element_type=F32)
        act = (0.5 * hidden * (1.0 + lax.erf(hidden * math.sqrt(0.5)))).astype(BF16)
        result = mid + lax.dot_general(
            act, w_down[...], (((1,), (1,)), ((), ())), preferred_element_type=F32
        )
        done[row] = result.reshape(n, feats, width)
        store(row).start()
        return carry

    lax.fori_loop(0, rows, finish, 0)

    for row in range(rows):
        settle(tok, send_sems, 0, row)
        settle(ctx, send_sems, 1, row)
        store(row).wait()


def body(
    cells, missing, feat_ids, feat_table, nan_embed, gain_one, w_qkv, w_out, gain_two, w_up, w_down
):
    n = lax.axis_size("feat")
    all_rows, feats, width = cells.shape
    rows = all_rows // n
    packed = width == 192 and feats % 32 == 0
    piece = (feats + feats // 2, 128) if packed else (feats, width)
    buffer = pltpu.VMEM((rows, n) + piece, BF16)
    operands = (
        cells.reshape(n, rows, feats, width),
        missing.T,
        feat_ids[None],
        feat_table,
        nan_embed[None],
        gain_one[None],
        w_qkv,
        w_out,
        gain_two[None],
        w_up,
        w_down.T,
    )
    result = pl.pallas_call(
        functools.partial(kernel, n, rows, feats, width, packed),
        out_shape=jax.ShapeDtypeStruct((n, rows, feats, width), F32),
        in_specs=[pl.BlockSpec(memory_space=pltpu.HBM)] * len(operands),
        out_specs=pl.BlockSpec(memory_space=pltpu.HBM),
        scratch_shapes=[pltpu.VMEM(x.shape, x.dtype) for x in operands]
        + [
            buffer,
            buffer,
            buffer,
            buffer,
            pltpu.VMEM((2 * width, width), BF16),
            pltpu.VMEM((rows, n, feats, width), F32),
            pltpu.SemaphoreType.DMA((len(operands),)),
            pltpu.SemaphoreType.DMA((2, rows)),
            pltpu.SemaphoreType.DMA((2, rows)),
            pltpu.SemaphoreType.DMA((rows,)),
        ],
        compiler_params=pltpu.CompilerParams(
            collective_id=0, has_side_effects=True, vmem_limit_bytes=LIMIT
        ),
    )(*operands)
    return result.reshape(all_rows, feats, width)


def solution(mesh):
    in_specs = (
        P("groups", "feat", None),
        P("groups", "feat"),
        P(("groups", "feat")),
        P(),
        P(),
        P(),
        P(),
        P(),
        P(),
        P(),
        P(),
    )
    out_specs = P("groups", "feat", None)
    return jax.shard_map(body, mesh=mesh, in_specs=in_specs, out_specs=out_specs, check_vma=False)
```
